128 devices in a mesh: gz: 32 (over y_lo, z, x), col: 4 (over y_hi, core).
Axes of the slice: x: 4, y: 4 (y_hi: 2, y_lo: 2; y = y_hi * 2 + y_lo), z: 4, core: 2. Of those that a mesh axis runs over, the one named last changes fastest.
Arguments:
- features: bfloat16 [64, 64, 128, 128], P(None, 'gz'), may hold values from -6 to 6
- grad_out: bfloat16 [64, 64, 128, 128], P('col', 'gz'), may hold values from -6 to 6
- conv_weight: bfloat16 [64, 64, 27], P('col'), may hold values from -0.15625 to 0.15625
- spectral_weight: bfloat16 [64, 64, 16, 256], P(None, 'col', None, 'gz'), may hold values from -3 to 3
Outputs:
- layer_out: bfloat16 [64, 64, 128, 128], P('col', 'gz')
- grad_input: bfloat16 [64, 64, 128, 128], P('col', 'gz')
- grad_conv: float32 [64, 64, 27], P('col')
- grad_spectral: float32 [64, 64, 16, 256], P(None, 'col', None, 'gz')
The draws below stay inside these ranges and needn't reach their ends.
All inputs are finite; a program needn't handle non-finite values.
Results may differ from the reference program's by a relative error of at most 0.008.
Values may be sent and summed in bfloat16 or wider, within the bound.
No kernel may reach another device: no remote copies, remote signals or barrier semaphores. Data moves between devices by JAX's collectives and lax.ppermute only.
A program may use at most 256 MiB of HBM per device.

```python
import math
from functools import partial
import jax
import jax.numpy as jnp
from jax import lax

WIDTH = 64
NX = 128
NY = 128
MODES = 16
NZ = 64


def block_levels(own_key, shape, cuts, low, largest):
    level = 1.0
    for position, shards_of in cuts:
        heights = jax.random.uniform(jax.random.fold_in(jax.random.fold_in(own_key, 6), position), (shards_of,), jnp.float32, low / len(cuts), largest / len(cuts))
        level = level * jnp.repeat(jnp.exp(heights), shape[position] // shards_of).reshape((-1,) + (1,) * (len(shape) - 1 - position))
    return level


def centred(key, extent, scale, bound, split=(), kind=jnp.bfloat16):
    result = scale * jax.random.normal(key, extent, jnp.float32)
    if split:
        result = result * block_levels(key, extent, split, -0.22, 0.18)
    return jnp.clip(result, -bound, bound).astype(kind)


def setup_inputs(seed: int = 0) -> dict:
    arg_keys = jax.random.split(jax.random.key(seed), 5)
    return {
        "features": centred(arg_keys[0], (WIDTH, NZ, NX, NY), 1.0, 6.0, ((1, 32),)),
        "grad_out": centred(arg_keys[1], (WIDTH, NZ, NX, NY), 1.0, 6.0, ((0, 4), (1, 32))),
        "conv_weight": centred(arg_keys[2], (WIDTH, WIDTH, 27), (27 * WIDTH) ** -0.5, 0.15625, ((0, 4),)),
        "spectral_weight": centred(arg_keys[3], (WIDTH, WIDTH, MODES, MODES * MODES), 0.5, 3.0, ((1, 4), (3, 32))),
    }


highest = lax.Precision.HIGHEST

def basis(length, mode_count):
    indices = jnp.arange(mode_count, dtype=jnp.int32)
    middle = mode_count // 2
    cosine_rows = indices <= middle
    frequency = jnp.where(cosine_rows, indices, indices - middle)
    positions = jnp.arange(length, dtype=jnp.int32)
    residue = frequency[:, None] * positions[None, :] % length
    radians = residue.astype(jnp.float32) * (2.0 * math.pi / length)
    tables = jnp.where(cosine_rows[:, None], jnp.cos(radians), jnp.sin(radians))
    return tables * math.sqrt(2.0 / length)

def activate(preact, cotangent):
    outcome, pullback = jax.vjp(partial(jax.nn.gelu, approximate=True), preact)
    return (outcome, pullback(cotangent)[0])

def shift_of(offset, direction):
    return (direction * (1 - offset // 9), direction * (1 - offset // 3 % 3), direction * (1 - offset % 3))

def reference(features, grad_out, conv_weight, spectral_weight):
    table_x = basis(NX, MODES)
    table_y = basis(NY, MODES)
    table_z = basis(NZ, MODES)
    cell_count = NZ * NX * NY

    def analyse(volume):
        along_y = jnp.dot(volume.reshape(WIDTH * NZ * NX, NY), table_y.astype(jnp.bfloat16).T, preferred_element_type=jnp.float32)
        along_y = along_y.reshape(WIDTH, NZ, NX, MODES)
        along_x = jnp.einsum('kx,czxl->czkl', table_x, along_y, precision=highest)
        along_z = jnp.einsum('jz,czkl->cjkl', table_z, along_x, precision=highest)
        return along_z.reshape(WIDTH, MODES, MODES * MODES)

    def synthesise(spectrum):
        blocks = spectrum.reshape(WIDTH, MODES, MODES, MODES)
        along_z = jnp.einsum('jz,cjkl->czkl', table_z, blocks, precision=highest)
        along_x = jnp.einsum('kx,czkl->czxl', table_x, along_z, precision=highest)
        return jnp.einsum('czxl,ly->czxy', along_x, table_y, precision=highest)
    conv_sum = jnp.zeros((WIDTH, cell_count), jnp.float32)
    for offset in range(27):
        moved = jnp.roll(features, shift_of(offset, 1), axis=(1, 2, 3)).reshape(WIDTH, cell_count)
        conv_sum = conv_sum + jnp.dot(conv_weight[:, :, offset], moved, preferred_element_type=jnp.float32)
    weights32 = spectral_weight.astype(jnp.float32)
    spectrum = analyse(features)
    mixed = jnp.einsum('iokm,ikm->okm', weights32, spectrum, precision=highest)
    preact = conv_sum.reshape(WIDTH, NZ, NX, NY) + synthesise(mixed)
    outcome, slope = activate(preact, grad_out.astype(jnp.float32))
    layer_out = outcome.astype(jnp.bfloat16)
    grad_pre = slope.astype(jnp.bfloat16)
    flat_grad = grad_pre.reshape(WIDTH, cell_count)
    back_conv = jnp.zeros((WIDTH, cell_count), jnp.float32)
    kernel_grads = []
    for offset in range(27):
        moved_grad = jnp.roll(grad_pre, shift_of(offset, -1), axis=(1, 2, 3)).reshape(WIDTH, cell_count)
        back_conv = back_conv + jnp.dot(conv_weight[:, :, offset].T, moved_grad, preferred_element_type=jnp.float32)
        moved = jnp.roll(features, shift_of(offset, 1), axis=(1, 2, 3)).reshape(WIDTH, cell_count)
        kernel_grads.append(lax.dot_general(flat_grad, moved, (((1,), (1,)), ((), ())), preferred_element_type=jnp.float32))
    scaling = 1.0 / math.sqrt(NX * NY * NZ)
    grad_conv = jnp.stack(kernel_grads, axis=2) * scaling
    grad_modes = analyse(grad_pre)
    back_modes = jnp.einsum('iokm,okm->ikm', weights32, grad_modes, precision=highest)
    grad_input = (back_conv.reshape(WIDTH, NZ, NX, NY) + synthesise(back_modes)).astype(jnp.bfloat16)
    grad_spectral = spectrum[:, None] * grad_modes[None]
    return (layer_out, grad_input, grad_conv, grad_spectral)
```

```python
import math

import jax
import jax.numpy as jnp
from jax import lax
from jax.experimental import pallas as pl
from jax.experimental.pallas import tpu as pltpu
from jax.sharding import PartitionSpec as P

highest = lax.Precision.HIGHEST
f32 = jnp.float32
bf16 = jnp.bfloat16
SIDE = 128
OWN = 16
ALL = 64
UNROLL = 8
GELU_A = math.sqrt(2.0 / math.pi)
GELU_B = 0.044715

PLANE_TERMS = (((0, 2),), ((0, 1), (1, 2)), ((0, 0), (1, 1)), ((1, 0),))


def basis(length, mode_count):
    indices = jnp.arange(mode_count, dtype=jnp.int32)
    middle = mode_count // 2
    cosine_rows = indices <= middle
    frequency = jnp.where(cosine_rows, indices, indices - middle)
    positions = jnp.arange(length, dtype=jnp.int32)
    residue = frequency[:, None] * positions[None, :] % length
    radians = residue.astype(jnp.float32) * (2.0 * math.pi / length)
    tables = jnp.where(cosine_rows[:, None], jnp.cos(radians), jnp.sin(radians))
    return tables * math.sqrt(2.0 / length)


def split2(value):
    high = value.astype(bf16)
    low = (value - high.astype(f32)).astype(bf16)
    return high, low


def dot(a, b):
    return jnp.dot(a, b, preferred_element_type=f32)


def dot_nt(a, b):
    return lax.dot_general(a, b, (((1,), (1,)), ((), ())), preferred_element_type=f32)


def conv_rows(slab, w_ref, int_ref, rim_ref):
    def block(step, carry):
        w = w_ref[...]
        for u in range(UNROLL):
            x = step * UNROLL + u
            near = ((x + SIDE - 1) % SIDE, x, (x + 1) % SIDE)
            rhs = jnp.concatenate(
                [jnp.concatenate([slab(z, n) for n in near], axis=0) for z in range(2)], axis=1
            )
            r = dot(w, rhs)

            def part(z, a, c):
                row = (a * 3 + c) * OWN
                return r[row : row + OWN, z * SIDE : (z + 1) * SIDE]

            for plane, terms in enumerate(PLANE_TERMS):
                c0, c1, c2 = (sum(part(z, a, c) for z, a in terms) for c in range(3))
                total = c1 + pltpu.roll(c0, 1, axis=1) + pltpu.roll(c2, SIDE - 1, axis=1)
                if plane in (1, 2):
                    int_ref[pl.ds((plane - 1) * SIDE + x, OWN, stride=2 * SIDE), :] = total
                else:
                    rim_ref[pl.ds((plane // 3) * SIDE + x, OWN, stride=2 * SIDE), :] = total
        return carry

    lax.fori_loop(0, SIDE // UNROLL, block, 0)


def write_rims(rim_ref, low_ref, high_ref):
    def block(o, carry):
        low_ref[o] = rim_ref[pl.ds(o * 2 * SIDE, SIDE), :].astype(bf16)
        high_ref[o] = rim_ref[pl.ds(o * 2 * SIDE + SIDE, SIDE), :].astype(bf16)
        return carry

    lax.fori_loop(0, OWN, block, 0)


def forward_conv_kernel(f_ref, w_ref, xt_ref, int_ref, low_ref, high_ref, rim_ref, turn_ref):
    def turn(step, carry):
        for z in range(2):
            rows = f_ref[:, z, pl.ds(step * 16, 16), :].astype(f32)
            turn_ref[z] = rows.reshape(ALL * 16, SIDE)
        for z in range(2):
            for u in range(16):
                xt_ref[z, step * 16 + u] = turn_ref[z, pl.ds(u, ALL, stride=16), :].astype(bf16)
        return carry

    lax.fori_loop(0, SIDE // 16, turn, 0)
    conv_rows(lambda z, x: xt_ref[z, x], w_ref, int_ref, rim_ref)
    write_rims(rim_ref, low_ref, high_ref)


def forward_conv(features, w):
    return pl.pallas_call(
        forward_conv_kernel,
        out_shape=(
            jax.ShapeDtypeStruct((2, SIDE, ALL, SIDE), bf16),
            jax.ShapeDtypeStruct((OWN * 2 * SIDE, SIDE), f32),
            jax.ShapeDtypeStruct((OWN, SIDE, SIDE), bf16),
            jax.ShapeDtypeStruct((OWN, SIDE, SIDE), bf16),
        ),
        scratch_shapes=[
            pltpu.VMEM((OWN * 2 * SIDE, SIDE), f32),
            pltpu.VMEM((2, ALL * 16, SIDE), f32),
        ],
        name="forward_conv",
    )(features, w)


def back_conv_kernel(g0, g1, g2, g3, w_ref, int_ref, low_ref, high_ref, rim_ref):
    def slab(z, x):
        return jnp.concatenate([g[z, x] for g in (g0, g1, g2, g3)], axis=0)

    conv_rows(slab, w_ref, int_ref, rim_ref)
    write_rims(rim_ref, low_ref, high_ref)


def back_conv(shares, w):
    return pl.pallas_call(
        back_conv_kernel,
        out_shape=(
            jax.ShapeDtypeStruct((OWN * 2 * SIDE, SIDE), f32),
            jax.ShapeDtypeStruct((OWN, SIDE, SIDE), bf16),
            jax.ShapeDtypeStruct((OWN, SIDE, SIDE), bf16),
        ),
        scratch_shapes=[pltpu.VMEM((OWN * 2 * SIDE, SIDE), f32)],
        name="back_conv",
    )(*shares, w)


def finish_modes(g_ref, ey2, out_ref, width):
    for kx in range(16):
        high, low = split2(g_ref[kx * width : (kx + 1) * width, :])
        out_ref[kx * 16 : (kx + 1) * 16, :] = dot_nt(ey2, jnp.concatenate([high, low], axis=1))


def analyse_kernel(f_ref, ex2_ref, ey2_ref, out_ref, g_ref):
    def block(step, carry):
        ex2 = ex2_ref[...]
        for u in range(8):
            ch = step * 8 + u
            r = dot(ex2, jnp.concatenate([f_ref[ch, 0], f_ref[ch, 1]], axis=1))
            g = r[:16] + r[16:]
            g_ref[pl.ds(ch, 16, stride=2 * ALL), :] = g[:, :SIDE]
            g_ref[pl.ds(ch + ALL, 16, stride=2 * ALL), :] = g[:, SIDE:]
        return carry

    lax.fori_loop(0, ALL // 8, block, 0)
    finish_modes(g_ref, ey2_ref[...], out_ref, 2 * ALL)


def analyse(features, ex2, ey2):
    return pl.pallas_call(
        analyse_kernel,
        out_shape=jax.ShapeDtypeStruct((256, 2 * ALL), f32),
        scratch_shapes=[pltpu.VMEM((16 * 2 * ALL, SIDE), f32)],
        name="analyse",
    )(features, ex2, ey2)


def along_y(s_ref, eyh_ref, eyl_ref, t_ref):
    high, low = split2(s_ref[...])
    eyh = eyh_ref[...]
    t_ref[...] = dot(high, eyh) + dot(low, eyh) + dot(high, eyl_ref[...])


def along_x(t_ref, ext3, o):
    t = jnp.concatenate([t_ref[pl.ds(o * 32, 16), :], t_ref[pl.ds(o * 32 + 16, 16), :]], axis=1)
    high, low = split2(t)
    return dot(ext3, jnp.concatenate([high, high, low], axis=0))


def middle_kernel(
    int_ref, fl_ref, fh_ref, s_ref, go_ref, ex2_ref, ey2_ref, ext3_ref, eyh_ref, eyl_ref,
    out_ref, gt_ref, modes_ref, t_ref, g_ref, turn_ref,
):
    along_y(s_ref, eyh_ref, eyl_ref, t_ref)

    def block(o, carry):
        smooth = along_x(t_ref, ext3_ref[...], o)
        halves = []
        for z in range(2):
            rim = (fl_ref if z == 0 else fh_ref)[o].astype(f32)
            p = int_ref[pl.ds(o * 256 + z * SIDE, SIDE), :] + rim + smooth[:, z * SIDE : (z + 1) * SIDE]
            square = p * p
            t = jnp.tanh(GELU_A * p * (1.0 + GELU_B * square))
            half = 0.5 * (1.0 + t)
            out_ref[o, z] = (p * half).astype(bf16)
            slope = half + 0.5 * p * (1.0 - t * t) * (GELU_A * (1.0 + 3.0 * GELU_B * square))
            g = (go_ref[o, z].astype(f32) * slope).astype(bf16)
            halves.append(g)
            turn_ref[pl.ds(o * 256 + z * SIDE, SIDE), :] = g.astype(f32)
        r = dot(ex2_ref[...], jnp.concatenate(halves, axis=1))
        r = r[:16] + r[16:]
        g_ref[pl.ds(o, 16, stride=2 * OWN), :] = r[:, :SIDE]
        g_ref[pl.ds(o + OWN, 16, stride=2 * OWN), :] = r[:, SIDE:]
        return carry

    lax.fori_loop(0, OWN, block, 0)
    finish_modes(g_ref, ey2_ref[...], modes_ref, 2 * OWN)

    def turn(step, carry):
        for z in range(2):
            for u in range(UNROLL):
                x = step * UNROLL + u
                gt_ref[z, x] = turn_ref[pl.ds(z * SIDE + x, OWN, stride=2 * SIDE), :].astype(bf16)
        return carry

    lax.fori_loop(0, SIDE // UNROLL, turn, 0)


def middle(conv_int, from_low, from_high, slab, grad_out, tables):
    ex2, ey2, ext3, eyh, eyl = tables
    return pl.pallas_call(
        middle_kernel,
        out_shape=(
            jax.ShapeDtypeStruct((OWN, 2, SIDE, SIDE), bf16),
            jax.ShapeDtypeStruct((2, SIDE, OWN, SIDE), bf16),
            jax.ShapeDtypeStruct((256, 2 * OWN), f32),
        ),
        scratch_shapes=[
            pltpu.VMEM((OWN * 2 * 16, SIDE), f32),
            pltpu.VMEM((16 * 2 * OWN, SIDE), f32),
            pltpu.VMEM((OWN * 2 * SIDE, SIDE), f32),
        ],
        name="middle",
    )(conv_int, from_low, from_high, slab, grad_out, ex2, ey2, ext3, eyh, eyl)


def kernel_grad_kernel(xt_ref, gt_ref, gl_ref, gh_ref, out_ref):
    out_ref[...] = jnp.zeros_like(out_ref)

    def block(step, carry):
        lefts, rights = [], []
        for u in range(UNROLL):
            x = step * UNROLL + u
            near = ((x + SIDE - 1) % SIDE, x, (x + 1) % SIDE)
            for z in range(2):
                lefts.append(jnp.concatenate([xt_ref[z, n] for n in near], axis=0))
            planes = []
            for g in (gl_ref[x], gt_ref[0, x], gt_ref[1, x], gh_ref[x]):
                wide = g.astype(f32)
                planes.append((
                    pltpu.roll(wide, SIDE - 1, axis=1).astype(bf16),
                    g,
                    pltpu.roll(wide, 1, axis=1).astype(bf16),
                ))
            for z in range(2):
                rights.append(jnp.concatenate([planes[z - a + 2][c] for a in range(3) for c in range(3)], axis=0))
        out_ref[...] += dot_nt(jnp.concatenate(lefts, axis=1), jnp.concatenate(rights, axis=1))
        return carry

    lax.fori_loop(0, SIDE // UNROLL, block, 0)


def kernel_grad(xt, gt, gl, gh):
    return pl.pallas_call(
        kernel_grad_kernel,
        out_shape=jax.ShapeDtypeStruct((3 * ALL, 9 * OWN), f32),
        name="kernel_grad",
    )(xt, gt, gl, gh)


def last_kernel(int_ref, fl_ref, fh_ref, s_ref, ext3_ref, eyh_ref, eyl_ref, out_ref, t_ref):
    along_y(s_ref, eyh_ref, eyl_ref, t_ref)

    def block(o, carry):
        smooth = along_x(t_ref, ext3_ref[...], o)
        for z in range(2):
            rim = (fl_ref if z == 0 else fh_ref)[o].astype(f32)
            p = int_ref[pl.ds(o * 256 + z * SIDE, SIDE), :] + rim + smooth[:, z * SIDE : (z + 1) * SIDE]
            out_ref[o, z] = p.astype(bf16)
        return carry

    lax.fori_loop(0, OWN, block, 0)


def last(conv_int, from_low, from_high, slab, tables):
    _, _, ext3, eyh, eyl = tables
    return pl.pallas_call(
        last_kernel,
        out_shape=jax.ShapeDtypeStruct((OWN, 2, SIDE, SIDE), bf16),
        scratch_shapes=[pltpu.VMEM((OWN * 2 * 16, SIDE), f32)],
        name="last",
    )(conv_int, from_low, from_high, slab, ext3, eyh, eyl)


def ring(axis, step):
    count = lax.axis_size(axis)
    return [(i, (i + step) % count) for i in range(count)]


def swap(value, bits):
    count = lax.axis_size("col")
    return lax.ppermute(value, "col", [(i, i ^ bits) for i in range(count)])


def to_slabs(mixed, table_z):
    columns = jnp.einsum("jz,cjm->czm", table_z, mixed, precision=highest)
    slabs = lax.all_to_all(columns, "gz", split_axis=1, concat_axis=2, tiled=True)
    return slabs.reshape(OWN * 2 * 16, 16)


def sum_over_slabs(value):
    def stage(value, period, stride):
        count = lax.axis_size("gz")
        total = value
        for k in range(1, period):
            pairs = []
            for i in range(count):
                digit = i // stride % period
                pairs.append((i, i + ((digit + k) % period - digit) * stride))
            total = total + lax.ppermute(value, "gz", pairs)
        return total

    return stage(stage(stage(value, 4, 1), 4, 4), 2, 16)


def local(features, grad_out, conv_weight, spectral_weight):
    plane_count = features.shape[1]
    groups = lax.axis_size("gz")
    table_x = basis(SIDE, 16)
    table_y = basis(SIDE, 16)
    table_z = basis(plane_count * groups, 16)
    exh, exl = split2(table_x)
    eyh, eyl = split2(table_y)
    ex2 = jnp.concatenate([exh, exl], axis=0)
    ey2 = jnp.concatenate([eyh, eyh], axis=1)
    ext3 = jnp.concatenate([exh.T, exl.T, exh.T], axis=1)
    tables = (ex2, ey2, ext3, eyh, eyl)
    first = lax.axis_index("col") * OWN

    kernel = conv_weight.reshape(OWN, ALL, 3, 3, 3)
    w_forward = jnp.transpose(kernel, (2, 4, 0, 3, 1)).reshape(9 * OWN, 3 * ALL)
    pieces = []
    for bits in range(4):
        there = jnp.bitwise_xor(lax.axis_index("col"), bits) * OWN
        piece = lax.dynamic_slice_in_dim(conv_weight, there, OWN, 1)
        pieces.append(swap(piece, bits) if bits else piece)
    back = jnp.stack(pieces).reshape(4, OWN, OWN, 3, 3, 3)[:, :, :, ::-1, ::-1, ::-1]
    w_back = jnp.transpose(back, (3, 5, 2, 4, 0, 1)).reshape(9 * OWN, 3 * ALL)

    xt, conv_int, rim_low, rim_high = forward_conv(features, w_forward)
    up, down = ring("gz", 1), ring("gz", -1)
    from_low = lax.ppermute(rim_high, "gz", up)
    from_high = lax.ppermute(rim_low, "gz", down)

    planes = analyse(features, ex2, ey2)
    planes = lax.all_to_all(planes.reshape(groups, 8, 2 * ALL), "gz", 0, 0, tiled=True)
    table_gz = table_z.reshape(16, groups, plane_count)
    spectrum = jnp.einsum(
        "jgz,gmzc->cjm", table_gz, planes.reshape(groups, 8, plane_count, ALL), precision=highest
    )
    weights32 = spectral_weight.astype(f32)
    mixed = jnp.sum(weights32 * spectrum[:, None], axis=0)
    slab = to_slabs(mixed, table_z)
    layer_out, gt, grad_planes = middle(conv_int, from_low, from_high, slab, grad_out, tables)

    g_low = lax.ppermute(gt[1], "gz", up)
    g_high = lax.ppermute(gt[0], "gz", down)
    g1 = swap(gt, 1)
    g2 = swap(gt, 2)
    g3 = swap(g2, 1)

    grad_planes = lax.all_to_all(grad_planes.reshape(groups, 8, 2 * OWN), "gz", 0, 0, tiled=True)
    grad_modes = jnp.einsum(
        "jgz,gmzc->cjm", table_gz, grad_planes.reshape(groups, 8, plane_count, OWN), precision=highest
    )
    grad_spectral = spectrum[:, None] * grad_modes[None]
    back_terms = jnp.sum(weights32 * grad_modes[None], axis=1)

    local_grad = sum_over_slabs(kernel_grad(xt, gt, g_low, g_high))
    back_int, back_low, back_high = back_conv((gt, g1, g2, g3), w_back)
    back_from_low = lax.ppermute(back_high, "gz", up)
    back_from_high = lax.ppermute(back_low, "gz", down)

    back_modes = lax.dynamic_slice_in_dim(back_terms, first, OWN, 0)
    for bits in range(1, 4):
        there = jnp.bitwise_xor(lax.axis_index("col"), bits) * OWN
        back_modes = back_modes + swap(lax.dynamic_slice_in_dim(back_terms, there, OWN, 0), bits)
    grad_input = last(back_int, back_from_low, back_from_high, to_slabs(back_modes, table_z), tables)

    scaling = 1.0 / math.sqrt(SIDE * SIDE * plane_count * groups)
    grad_conv = jnp.transpose(local_grad.reshape(3, ALL, 3, 3, OWN), (4, 1, 2, 0, 3)).reshape(OWN, ALL, 27) * scaling
    return (layer_out, grad_input, grad_conv, grad_spectral)


def solution(mesh):
    return jax.shard_map(
        local,
        mesh=mesh,
        in_specs=(
            P(None, "gz", None, None),
            P("col", "gz", None, None),
            P("col", None, None),
            P(None, "col", None, "gz"),
        ),
        out_specs=(
            P("col", "gz", None, None),
            P("col", "gz", None, None),
            P("col", None, None),
            P(None, "col", None, "gz"),
        ),
        check_vma=False,
    )
```

```python
import math

import jax
import jax.numpy as jnp
import numpy as np
from jax import lax
from jax.experimental import pallas as pl
from jax.experimental.pallas import tpu as pltpu
from jax.sharding import PartitionSpec as P

highest = lax.Precision.HIGHEST
f32 = jnp.float32
bf16 = jnp.bfloat16
SIDE = 128
OWN = 16
ALL = 64
STRIP = 16
STRIPS = SIDE // STRIP
CHUNKS = 4
CONV_FLOPS = 2 * 27 * ALL * OWN * 2 * SIDE * SIDE
GELU_A = math.sqrt(2.0 / math.pi)
GELU_B = 0.044715


def basis(length, mode_count):
    indices = np.arange(mode_count)
    middle = mode_count // 2
    frequency = np.where(indices <= middle, indices, indices - middle)
    radians = frequency[:, None] * np.arange(length)[None, :] % length * (2.0 * math.pi / length)
    tables = np.where((indices <= middle)[:, None], np.cos(radians), np.sin(radians))
    return (tables * math.sqrt(2.0 / length)).astype(np.float32)


def host_split(table):
    high = table.astype(bf16)
    return high, (table - high.astype(np.float32)).astype(bf16)


def call(kernel, grid, ins, outs, scratch, *args):
    def spec(entry, shape):
        if entry == "hbm":
            return pl.BlockSpec(memory_space=pl.ANY)
        if entry is None:
            return pl.BlockSpec(shape, lambda k: (0,) * len(shape))
        return pl.BlockSpec(*entry)

    result = pl.pallas_call(
        kernel,
        grid=(grid,),
        in_specs=[spec(entry, value.shape) for entry, value in zip(ins, args)],
        out_specs=tuple(spec(entry, shape) for shape, _, entry in outs),
        out_shape=tuple(jax.ShapeDtypeStruct(shape, dtype) for shape, dtype, _ in outs),
        scratch_shapes=scratch,
        cost_estimate=pl.CostEstimate(flops=CONV_FLOPS, bytes_accessed=8 << 20, transcendentals=0),
        compiler_params=pltpu.CompilerParams(dimension_semantics=("arbitrary",)),
    )(*args)
    return result if len(outs) > 1 else result[0]


def whole(kernel, ins, outs, scratch, *args):
    def spec(kind):
        return pl.BlockSpec(memory_space=pl.ANY) if kind == "hbm" else pl.BlockSpec()

    def held(kind, value):
        space = {"vmem": pltpu.VMEM, "hbm": pltpu.HBM}.get(kind)
        return value if space is None else pltpu.with_memory_space_constraint(value, space)

    result = pl.pallas_call(
        kernel,
        in_specs=[spec(kind) for kind in ins],
        out_specs=tuple(spec(kind) for _, _, kind in outs),
        out_shape=tuple(
            pltpu.VMEM(shape, dtype) if kind == "vmem" else jax.ShapeDtypeStruct(shape, dtype)
            for shape, dtype, kind in outs
        ),
        scratch_shapes=scratch,
        cost_estimate=pl.CostEstimate(flops=CONV_FLOPS, bytes_accessed=8 << 20, transcendentals=0),
        compiler_params=pltpu.CompilerParams(vmem_limit_bytes=24 << 20),
    )(*(held(kind, value) for kind, value in zip(ins, args)))
    return result if len(outs) > 1 else result[0]


def chunk_copy(source, target, sem, k, size):
    rows = pl.ds(k * size, size)
    return pltpu.make_async_copy(source.at[rows], target.at[rows], sem.at[k])


def split2(value):
    high = value.astype(bf16)
    low = (value - high.astype(f32)).astype(bf16)
    return high, low


def dot(a, b):
    return jnp.dot(a, b, preferred_element_type=f32)


def dot_nt(a, b):
    return lax.dot_general(a, b, (((1,), (1,)), ((), ())), preferred_element_type=f32)


def fetch(sources, targets, sems):
    def copy(n, k):
        rows = pl.ds(k * STRIP, STRIP)
        return pltpu.make_async_copy(sources[n].at[:, rows], targets[n].at[:, rows], sems.at[n, k])

    def start(k):
        for n in range(len(sources)):
            copy(n, k).start()

    def wait(k):
        for n in range(len(sources)):
            copy(n, k).wait()

    step = pl.program_id(0)

    @pl.when(step == 0)
    def _():
        for k in (STRIPS - 1, *range(STRIPS - 1)):
            start(k)
        wait(STRIPS - 1)
        wait(0)

    @pl.when(step < STRIPS - 2)
    def _():
        wait(step + 1)


def conv_strip(slab, strip, w_ref, planes, turn_ref, flip):
    rows = 3 * OWN
    needed = []
    for z in range(2):
        offsets = [a for a in range(3) if (z + a - 1 if flip else z - a + 1) in planes]
        needed.append((min(offsets), max(offsets) + 1))
    for u in range(0, STRIP, 2):
        sums = {}
        for z in range(2):
            columns = []
            for v in range(2):
                x = strip * STRIP + u + v
                near = [(x + SIDE - 1) % SIDE, x, (x + 1) % SIDE]
                columns.append(jnp.concatenate([slab(z, n) for n in (near[::-1] if flip else near)], axis=0))
            low, high = needed[z]
            r = dot(w_ref[low * rows : high * rows, :], jnp.concatenate(columns, axis=1))
            for a in range(low, high):
                plane = z + a - 1 if flip else z - a + 1
                term = r[(a - low) * rows : (a - low + 1) * rows]
                sums[plane] = sums[plane] + term if plane in sums else term
        for place, plane in enumerate(planes):
            for v in range(2):
                half = sums[plane][:, v * SIDE : (v + 1) * SIDE]
                c0, c1, c2 = (half[c * OWN : (c + 1) * OWN] for c in range(3))
                if flip:
                    c0, c2 = c2, c0
                total = c1 + pltpu.roll(c0, 1, axis=1) + pltpu.roll(c2, SIDE - 1, axis=1)
                turn_ref[pl.ds(place * OWN * STRIP + u + v, OWN, stride=STRIP), :] = total


def turned(turn_ref, place):
    size = OWN * STRIP
    return turn_ref[place * size : (place + 1) * size, :].reshape(OWN, STRIP, SIDE)


def front_kernel(f_ref, w_ref, xt_ref, int_ref, low_ref, high_ref, field_ref, wide_ref, turn_ref):
    step = pl.program_id(0)

    @pl.when(step < STRIPS)
    def _():
        for z in range(2):
            wide_ref[z] = f_ref[:, z].astype(f32).reshape(ALL * STRIP, SIDE)
        for z in range(2):
            for u in range(STRIP):
                row = wide_ref[z, pl.ds(u, ALL, stride=STRIP), :].astype(bf16)
                field_ref[z, step * STRIP + u] = row
                xt_ref[z, u] = row

    @pl.when(step >= 2)
    def _():
        strip = lax.rem(step - 1, STRIPS)
        conv_strip(lambda z, x: field_ref[z, x], strip, w_ref, (-1, 0, 1, 2), turn_ref, False)
        write_strip(turn_ref, int_ref, low_ref, high_ref)


def write_strip(turn_ref, int_ref, low_ref, high_ref):
    low_ref[...] = turned(turn_ref, 0).astype(bf16)
    for z in range(2):
        int_ref[:, z] = turned(turn_ref, z + 1).astype(bf16)
    high_ref[...] = turned(turn_ref, 3).astype(bf16)


def front(features, w):
    def late(k):
        return lax.select(k < 2, 1, lax.rem(k - 1, STRIPS))

    def early(k):
        return jnp.minimum(k, STRIPS - 1)

    rim = ((OWN, SIDE, SIDE), bf16, ((OWN, STRIP, SIDE), lambda k: (0, late(k), 0)))
    return call(
        front_kernel, STRIPS + 2,
        (((ALL, 2, STRIP, SIDE), lambda k: (0, 0, early(k), 0)), None),
        (
            ((2, SIDE, ALL, SIDE), bf16, ((2, STRIP, ALL, SIDE), lambda k: (0, early(k), 0, 0))),
            ((OWN, 2, SIDE, SIDE), bf16, ((OWN, 2, STRIP, SIDE), lambda k: (0, 0, late(k), 0))),
            rim,
            rim,
        ),
        [
            pltpu.VMEM((2, SIDE, ALL, SIDE), bf16),
            pltpu.VMEM((2, ALL * STRIP, SIDE), f32),
            pltpu.VMEM((4 * OWN * STRIP, SIDE), f32),
        ],
        features, w,
    )


INNER_OUT = ((OWN, 2, SIDE, SIDE), bf16, ((OWN, 2, STRIP, SIDE), lambda k: (0, 0, k, 0)))
RIM_OUT = ((OWN, SIDE, SIDE), bf16, ((OWN, STRIP, SIDE), lambda k: (0, k, 0)))


def back_conv_kernel(g0, g1, g2, g3, w_ref, int_ref, low_ref, high_ref, f0, f1, f2, f3, turn_ref, sems):
    fields = (f0, f1, f2, f3)
    fetch((g0, g1, g2, g3), fields, sems)

    def slab(z, x):
        return jnp.concatenate([f[z, x] for f in fields], axis=0)

    conv_strip(slab, pl.program_id(0), w_ref, (-1, 0, 1, 2), turn_ref, True)
    write_strip(turn_ref, int_ref, low_ref, high_ref)


def back_conv(shares, w):
    return call(
        back_conv_kernel, STRIPS, ("hbm", "hbm", "hbm", "hbm", None),
        (INNER_OUT, RIM_OUT, RIM_OUT),
        [pltpu.VMEM((2, SIDE, OWN, SIDE), bf16)] * 4
        + [pltpu.VMEM((4 * OWN * STRIP, SIDE), f32), pltpu.SemaphoreType.DMA((4, STRIPS))],
        *shares, w,
    )


def finish_modes(g_ref, ey2, out_ref, width):
    for kx in range(16):
        high, low = split2(g_ref[kx * width : (kx + 1) * width, :])
        out_ref[kx * 16 : (kx + 1) * 16, :width] = dot_nt(ey2, jnp.concatenate([high, low], axis=1))


def analyse_kernel(f_hbm, ex2_ref, ey2_ref, out_ref, f_ref, g_ref, sem):
    size = ALL // CHUNKS
    for k in range(CHUNKS):
        chunk_copy(f_hbm, f_ref, sem, k, size).start()

    def chunk(k, carry):
        chunk_copy(f_hbm, f_ref, sem, k, size).wait()
        ex2 = ex2_ref[...]
        for u in range(size):
            ch = k * size + u
            r = dot(ex2, jnp.concatenate([f_ref[ch, 0], f_ref[ch, 1]], axis=1))
            g = r[:16] + r[16:]
            g_ref[pl.ds(ch, 16, stride=2 * ALL), :] = g[:, :SIDE]
            g_ref[pl.ds(ch + ALL, 16, stride=2 * ALL), :] = g[:, SIDE:]
        return carry

    lax.fori_loop(0, CHUNKS, chunk, 0)
    finish_modes(g_ref, ey2_ref[...], out_ref, 2 * ALL)


def analyse(features, ex2, ey2):
    return whole(
        analyse_kernel, ("hbm", None, None), (((256, 2 * ALL), f32, None),),
        [
            pltpu.VMEM((ALL, 2, SIDE, SIDE), bf16),
            pltpu.VMEM((16 * 2 * ALL, SIDE), f32),
            pltpu.SemaphoreType.DMA((CHUNKS,)),
        ],
        features, ex2, ey2,
    )


def along_y(s_ref, eyh_ref, eyl_ref, t_ref):
    sides = [
        jnp.concatenate([s_ref[pl.ds(half * 2 + z, 16, stride=4), :] for half in range(2)], axis=1)
        for z in range(2)
    ]
    high, low = split2(jnp.concatenate(sides, axis=0))
    lane = lax.broadcasted_iota(jnp.int32, (32, 256), 1)
    channel = lane % SIDE // 8
    eyh = eyh_ref[...]
    eyl = eyl_ref[...]
    for o in range(OWN):
        keep = (channel == o).astype(bf16)
        own = high * keep
        t_ref[o * 32 : (o + 1) * 32, :] = dot(own, eyh) + dot(low * keep, eyh) + dot(own, eyl)


def along_x(t_ref, ext3, o):
    t = jnp.concatenate([t_ref[pl.ds(o * 32, 16), :], t_ref[pl.ds(o * 32 + 16, 16), :]], axis=1)
    high, low = split2(t)
    return dot(ext3, jnp.concatenate([high, high, low], axis=0))


def middle_kernel(
    int_hbm, go_hbm, fl_ref, fh_ref, s_ref, ex2_ref, ey2_ref, ext3_ref, eyh_ref, eyl_ref,
    out_hbm, gt_ref, first_ref, last_ref, modes_ref,
    int_ref, go_ref, out_ref, t_ref, g_ref, turn_ref, wide_ref, in_sem, go_sem, out_sem,
):
    size = OWN // CHUNKS
    for k in range(CHUNKS):
        chunk_copy(int_hbm, int_ref, in_sem, k, size).start()
        chunk_copy(go_hbm, go_ref, go_sem, k, size).start()
    along_y(s_ref, eyh_ref, eyl_ref, t_ref)

    def chunk(k, carry):
        chunk_copy(int_hbm, int_ref, in_sem, k, size).wait()
        chunk_copy(go_hbm, go_ref, go_sem, k, size).wait()
        for u in range(size):
            o = k * size + u
            smooth = along_x(t_ref, ext3_ref[...], o)
            halves = []
            for z in range(2):
                rim = (fl_ref if z == 0 else fh_ref)[o].astype(f32)
                p = int_ref[o, z].astype(f32) + rim + smooth[:, z * SIDE : (z + 1) * SIDE]
                square = p * p
                t = jnp.tanh(p * (GELU_A + GELU_A * GELU_B * square))
                half = 0.5 + 0.5 * t
                out_ref[o, z] = (p * half).astype(bf16)
                slope = half + p * (0.5 - 0.5 * (t * t)) * (GELU_A + 3.0 * GELU_A * GELU_B * square)
                g = (go_ref[o, z].astype(f32) * slope).astype(bf16)
                halves.append(g)
                turn_ref[pl.ds(o * 256 + z * SIDE, SIDE), :] = g.astype(f32)
            r = dot(ex2_ref[...], jnp.concatenate(halves, axis=1))
            r = r[:16] + r[16:]
            g_ref[pl.ds(o, 16, stride=2 * OWN), :] = r[:, :SIDE]
            g_ref[pl.ds(o + OWN, 16, stride=2 * OWN), :] = r[:, SIDE:]
        chunk_copy(out_ref, out_hbm, out_sem, k, size).start()
        return carry

    lax.fori_loop(0, CHUNKS, chunk, 0)
    finish_modes(g_ref, ey2_ref[...], wide_ref, 2 * OWN)
    quarters = [wide_ref[pl.ds(j, 64, stride=4), :][:, : 2 * OWN] for j in range(4)]
    modes_ref[...] = jnp.concatenate(quarters, axis=1)

    def turn(part, carry):
        for z in range(2):
            for u in range(STRIP):
                x = part * STRIP + u
                row = turn_ref[pl.ds(z * SIDE + x, OWN, stride=2 * SIDE), :].astype(bf16)
                gt_ref[z, x] = row
                (first_ref, last_ref)[z][x] = row
        return carry

    lax.fori_loop(0, STRIPS, turn, 0)
    for k in range(CHUNKS):
        chunk_copy(out_ref, out_hbm, out_sem, k, size).wait()


OWN_FIELD = (OWN, 2, SIDE, SIDE)


def middle(conv_int, from_low, from_high, slab, grad_out, tables):
    ex2, ey2, ext3, eyh, eyl = tables
    halo = ((SIDE, OWN, SIDE), bf16, None)
    return whole(
        middle_kernel, ("hbm", "hbm", "vmem", "vmem", None, None, None, None, None, None),
        ((OWN_FIELD, bf16, "hbm"), ((2, SIDE, OWN, SIDE), bf16, None), halo, halo, ((64, SIDE), f32, None)),
        [
            pltpu.VMEM(OWN_FIELD, bf16),
            pltpu.VMEM(OWN_FIELD, bf16),
            pltpu.VMEM(OWN_FIELD, bf16),
            pltpu.VMEM((OWN * 2 * 16, SIDE), f32),
            pltpu.VMEM((16 * 2 * OWN, SIDE), f32),
            pltpu.VMEM((OWN * 2 * SIDE, SIDE), f32),
            pltpu.VMEM((256, SIDE), f32),
            pltpu.SemaphoreType.DMA((CHUNKS,)),
            pltpu.SemaphoreType.DMA((CHUNKS,)),
            pltpu.SemaphoreType.DMA((CHUNKS,)),
        ],
        conv_int, grad_out, from_low, from_high, slab, ex2, ey2, ext3, eyh, eyl,
    )


def kernel_grad_kernel(xt_ref, gt_ref, gl_ref, gh_ref, out_ref, field_ref, sum_ref, sems):
    fetch([xt_ref], [field_ref], sems)
    step = pl.program_id(0)
    lefts, rights = [], []
    for u in range(STRIP):
        x = step * STRIP + u
        near = ((x + SIDE - 1) % SIDE, x, (x + 1) % SIDE)
        for z in range(2):
            lefts.append(jnp.concatenate([field_ref[z, n] for n in near], axis=0))
        planes = []
        for g in (gl_ref[u], gt_ref[0, u], gt_ref[1, u], gh_ref[u]):
            wide = g.astype(f32)
            planes.append((
                pltpu.roll(wide, SIDE - 1, axis=1).astype(bf16),
                g,
                pltpu.roll(wide, 1, axis=1).astype(bf16),
            ))
        for z in range(2):
            rights.append(jnp.concatenate([planes[z - a + 2][c] for a in range(3) for c in range(3)], axis=0))
    part = dot_nt(jnp.concatenate(rights, axis=1), jnp.concatenate(lefts, axis=1))

    @pl.when(step == 0)
    def _():
        sum_ref[...] = part

    @pl.when(step > 0)
    def _():
        sum_ref[...] += part

    @pl.when(step == STRIPS - 1)
    def _():
        tiles = []
        for offset in range(27):
            row = (offset // 9 * 3 + offset % 3) * OWN
            b = offset // 3 % 3
            tile = sum_ref[row : row + OWN, b * ALL : (b + 1) * ALL]
            tiles.append(jnp.concatenate([tile[:8], tile[8:]], axis=1))
        tiles.append(jnp.zeros((8, SIDE), f32))
        for n in range(14):
            out_ref[n * 16 : (n + 1) * 16, :] = jnp.concatenate(tiles[2 * n : 2 * n + 2], axis=0).astype(bf16)


def kernel_grad(xt, gt, gl, gh):
    halo = ((STRIP, OWN, SIDE), lambda k: (k, 0, 0))
    return call(
        kernel_grad_kernel, STRIPS,
        ("hbm", ((2, STRIP, OWN, SIDE), lambda k: (0, k, 0, 0)), halo, halo),
        (((14 * 16, SIDE), bf16, None),),
        [
            pltpu.VMEM((2, SIDE, ALL, SIDE), bf16),
            pltpu.VMEM((9 * OWN, 3 * ALL), f32),
            pltpu.SemaphoreType.DMA((1, STRIPS)),
        ],
        xt, gt, gl, gh,
    )


def last_kernel(
    int_hbm, fl_ref, fh_ref, s_ref, ext3_ref, eyh_ref, eyl_ref, out_hbm, int_ref, out_ref, t_ref, in_sem, out_sem
):
    size = OWN // CHUNKS
    for k in range(CHUNKS):
        chunk_copy(int_hbm, int_ref, in_sem, k, size).start()
    along_y(s_ref, eyh_ref, eyl_ref, t_ref)

    def chunk(k, carry):
        chunk_copy(int_hbm, int_ref, in_sem, k, size).wait()
        for u in range(size):
            o = k * size + u
            smooth = along_x(t_ref, ext3_ref[...], o)
            for z in range(2):
                rim = (fl_ref if z == 0 else fh_ref)[o].astype(f32)
                total = int_ref[o, z].astype(f32) + rim + smooth[:, z * SIDE : (z + 1) * SIDE]
                out_ref[o, z] = total.astype(bf16)
        chunk_copy(out_ref, out_hbm, out_sem, k, size).start()
        return carry

    lax.fori_loop(0, CHUNKS, chunk, 0)
    for k in range(CHUNKS):
        chunk_copy(out_ref, out_hbm, out_sem, k, size).wait()


def last(conv_int, from_low, from_high, slab, tables):
    _, _, ext3, eyh, eyl = tables
    return whole(
        last_kernel, ("hbm", "vmem", "vmem", None, None, None, None), ((OWN_FIELD, bf16, "hbm"),),
        [
            pltpu.VMEM(OWN_FIELD, bf16),
            pltpu.VMEM(OWN_FIELD, bf16),
            pltpu.VMEM((OWN * 2 * 16, SIDE), f32),
            pltpu.SemaphoreType.DMA((CHUNKS,)),
            pltpu.SemaphoreType.DMA((CHUNKS,)),
        ],
        conv_int, from_low, from_high, slab, ext3, eyh, eyl,
    )


def ring(axis, step):
    count = lax.axis_size(axis)
    return [(i, (i + step) % count) for i in range(count)]


def swap(value, bits):
    count = lax.axis_size("col")
    return lax.ppermute(value, "col", [(i, i ^ bits) for i in range(count)])


def exchange(value):
    return lax.all_to_all(value, "gz", 0, 0, tiled=True)


def columns_of(mixed, table_z, groups):
    columns = jnp.einsum("jz,cjm->zcm", table_z, mixed, precision=highest)
    return columns.reshape(groups, -1, SIDE)


def step(features, grad_out, conv_weight, spectral_weight):
    plane_count = features.shape[1]
    groups = lax.axis_size("gz")
    table_x = basis(SIDE, 16)
    table_y = basis(SIDE, 16)
    table_z = basis(plane_count * groups, 16)
    exh, exl = host_split(table_x)
    eyh, eyl = host_split(table_y)
    ex2 = np.concatenate([exh, exl], axis=0)
    ey2 = np.concatenate([eyh, eyh], axis=1)
    ext3 = np.concatenate([exh.T, exl.T, exh.T], axis=1)
    eyh, eyl = (np.repeat(t.reshape(2, 1, 8, SIDE), OWN, axis=1).reshape(256, SIDE) for t in (eyh, eyl))
    tables = (ex2, ey2, ext3, eyh, eyl)

    kernel = conv_weight.reshape(OWN, ALL, 3, 3, 3)
    w_forward = jnp.transpose(kernel, (2, 4, 0, 3, 1)).reshape(9 * OWN, 3 * ALL)
    pieces = jnp.stack([conv_weight] + [swap(conv_weight, bits) for bits in range(1, 4)])
    back = lax.dynamic_slice_in_dim(pieces, lax.axis_index("col") * OWN, OWN, 2)
    back = back.reshape(4, OWN, OWN, 3, 3, 3)
    w_back = jnp.transpose(back, (3, 5, 2, 4, 0, 1)).reshape(9 * OWN, 3 * ALL)

    planes = analyse(features, ex2, ey2)
    planes = exchange(planes.reshape(groups, 8, 2 * ALL))
    xt, conv_int, rim_low, rim_high = front(features, w_forward)
    up, down = ring("gz", 1), ring("gz", -1)
    from_low = lax.ppermute(rim_high, "gz", up)
    from_high = lax.ppermute(rim_low, "gz", down)

    table_gz = table_z.reshape(16, groups, plane_count)
    spectrum = jnp.einsum(
        "jgz,gmzc->cjm", table_gz, planes.reshape(groups, 8, plane_count, ALL), precision=highest
    )
    weights32 = spectral_weight.astype(f32)
    mixed = jnp.sum(weights32 * spectrum[:, None], axis=0)
    slab = exchange(columns_of(mixed, table_z, groups)).reshape(2 * groups, SIDE)
    conv_int, w_back = lax.optimization_barrier((conv_int, w_back))
    layer_out, gt, gt_first, gt_last, grad_planes = middle(conv_int, from_low, from_high, slab, grad_out, tables)

    g_low = lax.ppermute(gt_last, "gz", up)
    g_high = lax.ppermute(gt_first, "gz", down)
    g1 = swap(gt, 1)
    g2 = swap(gt, 2)
    local_grad = kernel_grad(xt, gt, g_low, g_high)
    local_grad = local_grad.reshape(groups, -1, SIDE)
    packed = jnp.concatenate([grad_planes.astype(bf16).reshape(groups, 2, SIDE), local_grad], axis=1)
    packed = exchange(packed)
    scaling = 1.0 / math.sqrt(SIDE * SIDE * plane_count * groups)
    grad_chunk = packed[:, 2:].astype(f32).sum(axis=0) * scaling
    grad_planes = packed[:, :2].astype(f32).reshape(groups, 2, 4, plane_count, OWN)
    g3 = swap(g2, 1)
    grad_modes = jnp.einsum("jgz,grmzc->cjrm", table_gz, grad_planes, precision=highest)
    grad_modes = grad_modes.reshape(OWN, 16, 8)
    back_terms = jnp.sum(weights32 * grad_modes[None], axis=1)
    first = lax.axis_index("col") * OWN
    back_modes = lax.dynamic_slice_in_dim(back_terms, first, OWN, 0)
    for bits in range(1, 4):
        there = jnp.bitwise_xor(lax.axis_index("col"), bits) * OWN
        back_modes = back_modes + swap(lax.dynamic_slice_in_dim(back_terms, there, OWN, 0), bits)
    back_int, back_low, back_high = back_conv((gt, g1, g2, g3), w_back)
    back_from_low = lax.ppermute(back_high, "gz", up)
    back_from_high = lax.ppermute(back_low, "gz", down)
    grad_spectral = spectrum[:, None] * grad_modes[None]

    columns = columns_of(back_modes, table_z, groups).astype(bf16)
    grad_chunk = jnp.broadcast_to(grad_chunk.astype(bf16), (groups, *grad_chunk.shape))
    packed = exchange(jnp.concatenate([columns, grad_chunk], axis=1))
    slab = packed[:, :2].astype(f32).reshape(2 * groups, SIDE)
    grad_input = last(back_int, back_from_low, back_from_high, slab, tables)

    kernel_sum = packed[:, 2:].astype(f32).reshape(28, 8, 2, ALL)[:27]
    grad_conv = jnp.transpose(kernel_sum, (2, 1, 3, 0)).reshape(OWN, ALL, 27)
    return (layer_out, grad_input, grad_conv, grad_spectral)


def solution(mesh):
    return jax.shard_map(
        step,
        mesh=mesh,
        in_specs=(
            P(None, "gz", None, None),
            P("col", "gz", None, None),
            P("col", None, None),
            P(None, "col", None, "gz"),
        ),
        out_specs=(
            P("col", "gz", None, None),
            P("col", "gz", None, None),
            P("col", None, None),
            P(None, "col", None, "gz"),
        ),
        check_vma=False,
    )
```

```python
import math

import jax
import jax.numpy as jnp
import numpy as np
from jax import lax
from jax.experimental import pallas as pl
from jax.experimental.pallas import tpu as pltpu
from jax.sharding import PartitionSpec as P


highest = lax.Precision.HIGHEST
f32 = jnp.float32
bf16 = jnp.bfloat16
SIDE = 128
OWN = 16
ALL = 64
STRIP = 16
STRIPS = SIDE // STRIP
CHUNKS = 4
CONV_FLOPS = 2 * 27 * ALL * OWN * 2 * SIDE * SIDE
GELU_A = math.sqrt(2.0 / math.pi)
GELU_B = 0.044715


def basis(length, mode_count):
    indices = np.arange(mode_count)
    middle = mode_count // 2
    frequency = np.where(indices <= middle, indices, indices - middle)
    radians = frequency[:, None] * np.arange(length)[None, :] % length * (2.0 * math.pi / length)
    tables = np.where((indices <= middle)[:, None], np.cos(radians), np.sin(radians))
    return (tables * math.sqrt(2.0 / length)).astype(np.float32)


def host_split(table):
    high = table.astype(bf16)
    return high, (table - high.astype(np.float32)).astype(bf16)


def call(kernel, grid, ins, outs, scratch, *args):
    def spec(entry, shape):
        if entry == "hbm":
            return pl.BlockSpec(memory_space=pl.ANY)
        if entry is None:
            return pl.BlockSpec(shape, lambda k: (0,) * len(shape))
        return pl.BlockSpec(*entry)

    result = pl.pallas_call(
        kernel,
        grid=(grid,),
        in_specs=[spec(entry, value.shape) for entry, value in zip(ins, args)],
        out_specs=tuple(spec(entry, shape) for shape, _, entry in outs),
        out_shape=tuple(jax.ShapeDtypeStruct(shape, dtype) for shape, dtype, _ in outs),
        scratch_shapes=scratch,
        cost_estimate=pl.CostEstimate(flops=CONV_FLOPS, bytes_accessed=8 << 20, transcendentals=0),
        compiler_params=pltpu.CompilerParams(dimension_semantics=("arbitrary",)),
    )(*args)
    return result if len(outs) > 1 else result[0]


def whole(kernel, ins, outs, scratch, *args):
    def spec(kind):
        return pl.BlockSpec(memory_space=pl.ANY) if kind == "hbm" else pl.BlockSpec()

    def held(kind, value):
        space = {"vmem": pltpu.VMEM, "hbm": pltpu.HBM}.get(kind)
        return value if space is None else pltpu.with_memory_space_constraint(value, space)

    result = pl.pallas_call(
        kernel,
        in_specs=[spec(kind) for kind in ins],
        out_specs=tuple(spec(kind) for _, _, kind in outs),
        out_shape=tuple(
            pltpu.VMEM(shape, dtype) if kind == "vmem" else jax.ShapeDtypeStruct(shape, dtype)
            for shape, dtype, kind in outs
        ),
        scratch_shapes=scratch,
        cost_estimate=pl.CostEstimate(flops=CONV_FLOPS, bytes_accessed=8 << 20, transcendentals=0),
        compiler_params=pltpu.CompilerParams(vmem_limit_bytes=24 << 20),
    )(*(held(kind, value) for kind, value in zip(ins, args)))
    return result if len(outs) > 1 else result[0]


def chunk_copy(source, target, sem, k, size):
    rows = pl.ds(k * size, size)
    return pltpu.make_async_copy(source.at[rows], target.at[rows], sem.at[k])


def split2(value):
    high = value.astype(bf16)
    low = (value - high.astype(f32)).astype(bf16)
    return high, low


def dot(a, b):
    return jnp.dot(a, b, preferred_element_type=f32)


def dot_nt(a, b):
    return lax.dot_general(a, b, (((1,), (1,)), ((), ())), preferred_element_type=f32)


def fetch(sources, targets, sems):
    def copy(n, k):
        rows = pl.ds(k * STRIP, STRIP)
        return pltpu.make_async_copy(sources[n].at[:, rows], targets[n].at[:, rows], sems.at[n, k])

    def start(k):
        for n in range(len(sources)):
            copy(n, k).start()

    def wait(k):
        for n in range(len(sources)):
            copy(n, k).wait()

    step = pl.program_id(0)

    @pl.when(step == 0)
    def _():
        for k in (STRIPS - 1, *range(STRIPS - 1)):
            start(k)
        wait(STRIPS - 1)
        wait(0)

    @pl.when(step < STRIPS - 2)
    def _():
        wait(step + 1)


def conv_strip(slab, strip, w_ref, planes, turn_ref, flip):
    rows = 3 * OWN
    needed = []
    for z in range(2):
        offsets = [a for a in range(3) if (z + a - 1 if flip else z - a + 1) in planes]
        needed.append((min(offsets), max(offsets) + 1))
    for u in range(0, STRIP, 2):
        sums = {}
        for z in range(2):
            columns = []
            for v in range(2):
                x = strip * STRIP + u + v
                near = [(x + SIDE - 1) % SIDE, x, (x + 1) % SIDE]
                columns.append(jnp.concatenate([slab(z, n) for n in (near[::-1] if flip else near)], axis=0))
            low, high = needed[z]
            r = dot(w_ref[low * rows : high * rows, :], jnp.concatenate(columns, axis=1))
            for a in range(low, high):
                plane = z + a - 1 if flip else z - a + 1
                term = r[(a - low) * rows : (a - low + 1) * rows]
                sums[plane] = sums[plane] + term if plane in sums else term
        for place, plane in enumerate(planes):
            for v in range(2):
                half = sums[plane][:, v * SIDE : (v + 1) * SIDE]
                c0, c1, c2 = (half[c * OWN : (c + 1) * OWN] for c in range(3))
                if flip:
                    c0, c2 = c2, c0
                total = c1 + pltpu.roll(c0, 1, axis=1) + pltpu.roll(c2, SIDE - 1, axis=1)
                turn_ref[pl.ds(place * OWN * STRIP + u + v, OWN, stride=STRIP), :] = total


def turned(turn_ref, place):
    size = OWN * STRIP
    return turn_ref[place * size : (place + 1) * size, :].reshape(OWN, STRIP, SIDE)


def front_kernel(f_ref, w_ref, xt_ref, int_ref, low_ref, high_ref, field_ref, wide_ref, turn_ref):
    step = pl.program_id(0)

    @pl.when(step < STRIPS)
    def _():
        for z in range(2):
            wide_ref[z] = f_ref[:, z].astype(f32).reshape(ALL * STRIP, SIDE)
        for z in range(2):
            for u in range(STRIP):
                row = wide_ref[z, pl.ds(u, ALL, stride=STRIP), :].astype(bf16)
                field_ref[z, step * STRIP + u] = row
                xt_ref[z, u] = row

    @pl.when(step >= 2)
    def _():
        strip = lax.rem(step - 1, STRIPS)
        conv_strip(lambda z, x: field_ref[z, x], strip, w_ref, (-1, 0, 1, 2), turn_ref, False)
        write_strip(turn_ref, int_ref, low_ref, high_ref)


def write_strip(turn_ref, int_ref, low_ref, high_ref):
    low_ref[...] = turned(turn_ref, 0).astype(bf16)
    for z in range(2):
        int_ref[:, z] = turned(turn_ref, z + 1).astype(bf16)
    high_ref[...] = turned(turn_ref, 3).astype(bf16)


def front(features, w):
    def late(k):
        return lax.select(k < 2, 1, lax.rem(k - 1, STRIPS))

    def early(k):
        return jnp.minimum(k, STRIPS - 1)

    rim = ((OWN, SIDE, SIDE), bf16, ((OWN, STRIP, SIDE), lambda k: (0, late(k), 0)))
    return call(
        front_kernel, STRIPS + 2,
        (((ALL, 2, STRIP, SIDE), lambda k: (0, 0, early(k), 0)), None),
        (
            ((2, SIDE, ALL, SIDE), bf16, ((2, STRIP, ALL, SIDE), lambda k: (0, early(k), 0, 0))),
            ((OWN, 2, SIDE, SIDE), bf16, ((OWN, 2, STRIP, SIDE), lambda k: (0, 0, late(k), 0))),
            rim,
            rim,
        ),
        [
            pltpu.VMEM((2, SIDE, ALL, SIDE), bf16),
            pltpu.VMEM((2, ALL * STRIP, SIDE), f32),
            pltpu.VMEM((4 * OWN * STRIP, SIDE), f32),
        ],
        features, w,
    )


INNER_OUT = ((OWN, 2, SIDE, SIDE), bf16, ((OWN, 2, STRIP, SIDE), lambda k: (0, 0, k, 0)))
RIM_OUT = ((OWN, SIDE, SIDE), bf16, ((OWN, STRIP, SIDE), lambda k: (0, k, 0)))


def back_conv_kernel(g0, g1, g2, g3, w_ref, int_ref, low_ref, high_ref, f0, f1, f2, f3, turn_ref, sems):
    fields = (f0, f1, f2, f3)
    fetch((g0, g1, g2, g3), fields, sems)

    def slab(z, x):
        return jnp.concatenate([f[z, x] for f in fields], axis=0)

    conv_strip(slab, pl.program_id(0), w_ref, (-1, 0, 1, 2), turn_ref, True)
    write_strip(turn_ref, int_ref, low_ref, high_ref)


def back_conv(shares, w):
    return call(
        back_conv_kernel, STRIPS, ("hbm", "hbm", "hbm", "hbm", None),
        (INNER_OUT, RIM_OUT, RIM_OUT),
        [pltpu.VMEM((2, SIDE, OWN, SIDE), bf16)] * 4
        + [pltpu.VMEM((4 * OWN * STRIP, SIDE), f32), pltpu.SemaphoreType.DMA((4, STRIPS))],
        *shares, w,
    )


def finish_modes(g_ref, ey2, out_ref, width):
    for kx in range(16):
        high, low = split2(g_ref[kx * width : (kx + 1) * width, :])
        out_ref[kx * 16 : (kx + 1) * 16, :width] = dot_nt(ey2, jnp.concatenate([high, low], axis=1))


def analyse_kernel(f_hbm, ex2_ref, ey2_ref, out_ref, f_ref, g_ref, sem):
    size = ALL // CHUNKS
    for k in range(CHUNKS):
        chunk_copy(f_hbm, f_ref, sem, k, size).start()

    def chunk(k, carry):
        chunk_copy(f_hbm, f_ref, sem, k, size).wait()
        ex2 = ex2_ref[...]
        for u in range(size):
            ch = k * size + u
            r = dot(ex2, jnp.concatenate([f_ref[ch, 0], f_ref[ch, 1]], axis=1))
            g = r[:16] + r[16:]
            g_ref[pl.ds(ch, 16, stride=2 * ALL), :] = g[:, :SIDE]
            g_ref[pl.ds(ch + ALL, 16, stride=2 * ALL), :] = g[:, SIDE:]
        return carry

    lax.fori_loop(0, CHUNKS, chunk, 0)
    finish_modes(g_ref, ey2_ref[...], out_ref, 2 * ALL)


def analyse(features, ex2, ey2):
    return whole(
        analyse_kernel, ("hbm", None, None), (((256, 2 * ALL), f32, None),),
        [
            pltpu.VMEM((ALL, 2, SIDE, SIDE), bf16),
            pltpu.VMEM((16 * 2 * ALL, SIDE), f32),
            pltpu.SemaphoreType.DMA((CHUNKS,)),
        ],
        features, ex2, ey2,
    )


def along_y(s_ref, eyh_ref, eyl_ref, t_ref):
    sides = [
        jnp.concatenate([s_ref[pl.ds(half * 2 + z, 16, stride=4), :] for half in range(2)], axis=1)
        for z in range(2)
    ]
    high, low = split2(jnp.concatenate(sides, axis=0))
    lane = lax.broadcasted_iota(jnp.int32, (32, 256), 1)
    channel = lane % SIDE // 8
    eyh = eyh_ref[...]
    eyl = eyl_ref[...]
    for o in range(OWN):
        keep = (channel == o).astype(bf16)
        own = high * keep
        t_ref[o * 32 : (o + 1) * 32, :] = dot(own, eyh) + dot(low * keep, eyh) + dot(own, eyl)


def along_x(t_ref, ext3, o):
    t = jnp.concatenate([t_ref[pl.ds(o * 32, 16), :], t_ref[pl.ds(o * 32 + 16, 16), :]], axis=1)
    high, low = split2(t)
    return dot(ext3, jnp.concatenate([high, high, low], axis=0))


def middle_kernel(
    int_hbm, go_hbm, fl_ref, fh_ref, s_ref, ex2_ref, ey2_ref, ext3_ref, eyh_ref, eyl_ref,
    out_hbm, gt_ref, first_ref, last_ref, modes_ref,
    int_ref, go_ref, out_ref, t_ref, g_ref, turn_ref, wide_ref, in_sem, go_sem, out_sem,
):
    size = OWN // CHUNKS
    for k in range(CHUNKS):
        chunk_copy(int_hbm, int_ref, in_sem, k, size).start()
        chunk_copy(go_hbm, go_ref, go_sem, k, size).start()
    along_y(s_ref, eyh_ref, eyl_ref, t_ref)

    def chunk(k, carry):
        chunk_copy(int_hbm, int_ref, in_sem, k, size).wait()
        chunk_copy(go_hbm, go_ref, go_sem, k, size).wait()
        for u in range(size):
            o = k * size + u
            smooth = along_x(t_ref, ext3_ref[...], o)
            halves = []
            for z in range(2):
                rim = (fl_ref if z == 0 else fh_ref)[o].astype(f32)
                p = int_ref[o, z].astype(f32) + rim + smooth[:, z * SIDE : (z + 1) * SIDE]
                square = p * p
                t = jnp.tanh(p * (GELU_A + GELU_A * GELU_B * square))
                half = 0.5 + 0.5 * t
                out_ref[o, z] = (p * half).astype(bf16)
                slope = half + p * (0.5 - 0.5 * (t * t)) * (GELU_A + 3.0 * GELU_A * GELU_B * square)
                g = (go_ref[o, z].astype(f32) * slope).astype(bf16)
                halves.append(g)
                turn_ref[pl.ds(o * 256 + z * SIDE, SIDE), :] = g.astype(f32)
            r = dot(ex2_ref[...], jnp.concatenate(halves, axis=1))
            r = r[:16] + r[16:]
            g_ref[pl.ds(o, 16, stride=2 * OWN), :] = r[:, :SIDE]
            g_ref[pl.ds(o + OWN, 16, stride=2 * OWN), :] = r[:, SIDE:]
        chunk_copy(out_ref, out_hbm, out_sem, k, size).start()
        return carry

    lax.fori_loop(0, CHUNKS, chunk, 0)
    finish_modes(g_ref, ey2_ref[...], wide_ref, 2 * OWN)
    quarters = [wide_ref[pl.ds(j, 64, stride=4), :][:, : 2 * OWN] for j in range(4)]
    modes_ref[...] = jnp.concatenate(quarters, axis=1)

    def turn(part, carry):
        for z in range(2):
            for u in range(STRIP):
                x = part * STRIP + u
                row = turn_ref[pl.ds(z * SIDE + x, OWN, stride=2 * SIDE), :].astype(bf16)
                gt_ref[z, x] = row
                (first_ref, last_ref)[z][x] = row
        return carry

    lax.fori_loop(0, STRIPS, turn, 0)
    for k in range(CHUNKS):
        chunk_copy(out_ref, out_hbm, out_sem, k, size).wait()


OWN_FIELD = (OWN, 2, SIDE, SIDE)


def middle(conv_int, from_low, from_high, slab, grad_out, tables):
    ex2, ey2, ext3, eyh, eyl = tables
    halo = ((SIDE, OWN, SIDE), bf16, None)
    return whole(
        middle_kernel, ("hbm", "hbm", "vmem", "vmem", None, None, None, None, None, None),
        ((OWN_FIELD, bf16, "hbm"), ((2, SIDE, OWN, SIDE), bf16, None), halo, halo, ((64, SIDE), f32, None)),
        [
            pltpu.VMEM(OWN_FIELD, bf16),
            pltpu.VMEM(OWN_FIELD, bf16),
            pltpu.VMEM(OWN_FIELD, bf16),
            pltpu.VMEM((OWN * 2 * 16, SIDE), f32),
            pltpu.VMEM((16 * 2 * OWN, SIDE), f32),
            pltpu.VMEM((OWN * 2 * SIDE, SIDE), f32),
            pltpu.VMEM((256, SIDE), f32),
            pltpu.SemaphoreType.DMA((CHUNKS,)),
            pltpu.SemaphoreType.DMA((CHUNKS,)),
            pltpu.SemaphoreType.DMA((CHUNKS,)),
        ],
        conv_int, grad_out, from_low, from_high, slab, ex2, ey2, ext3, eyh, eyl,
    )


def kernel_grad_kernel(xt_ref, gt_ref, gl_ref, gh_ref, out_ref, field_ref, sum_ref, sems):
    fetch([xt_ref], [field_ref], sems)
    step = pl.program_id(0)
    lefts, rights = [], []
    for u in range(STRIP):
        x = step * STRIP + u
        near = ((x + SIDE - 1) % SIDE, x, (x + 1) % SIDE)
        for z in range(2):
            lefts.append(jnp.concatenate([field_ref[z, n] for n in near], axis=0))
        planes = []
        for g in (gl_ref[u], gt_ref[0, u], gt_ref[1, u], gh_ref[u]):
            wide = g.astype(f32)
            planes.append((
                pltpu.roll(wide, SIDE - 1, axis=1).astype(bf16),
                g,
                pltpu.roll(wide, 1, axis=1).astype(bf16),
            ))
        for z in range(2):
            rights.append(jnp.concatenate([planes[z - a + 2][c] for a in range(3) for c in range(3)], axis=0))
    part = dot_nt(jnp.concatenate(rights, axis=1), jnp.concatenate(lefts, axis=1))

    @pl.when(step == 0)
    def _():
        sum_ref[...] = part

    @pl.when(step > 0)
    def _():
        sum_ref[...] += part

    @pl.when(step == STRIPS - 1)
    def _():
        tiles = []
        for offset in range(27):
            row = (offset // 9 * 3 + offset % 3) * OWN
            b = offset // 3 % 3
            tile = sum_ref[row : row + OWN, b * ALL : (b + 1) * ALL]
            tiles.append(jnp.concatenate([tile[:8], tile[8:]], axis=1))
        tiles += [jnp.zeros((8, SIDE), f32)] * 5
        for n in range(16):
            out_ref[n * 16 : (n + 1) * 16, :] = jnp.concatenate(tiles[2 * n : 2 * n + 2], axis=0).astype(bf16)


def kernel_grad(xt, gt, gl, gh):
    halo = ((STRIP, OWN, SIDE), lambda k: (k, 0, 0))
    return call(
        kernel_grad_kernel, STRIPS,
        ("hbm", ((2, STRIP, OWN, SIDE), lambda k: (0, k, 0, 0)), halo, halo),
        (((32 * 8, SIDE), bf16, None),),
        [
            pltpu.VMEM((2, SIDE, ALL, SIDE), bf16),
            pltpu.VMEM((9 * OWN, 3 * ALL), f32),
            pltpu.SemaphoreType.DMA((1, STRIPS)),
        ],
        xt, gt, gl, gh,
    )


def last_kernel(
    int_hbm, fl_ref, fh_ref, s_ref, ext3_ref, eyh_ref, eyl_ref, out_hbm, int_ref, out_ref, t_ref, in_sem, out_sem
):
    size = OWN // CHUNKS
    for k in range(CHUNKS):
        chunk_copy(int_hbm, int_ref, in_sem, k, size).start()
    along_y(s_ref, eyh_ref, eyl_ref, t_ref)

    def chunk(k, carry):
        chunk_copy(int_hbm, int_ref, in_sem, k, size).wait()
        for u in range(size):
            o = k * size + u
            smooth = along_x(t_ref, ext3_ref[...], o)
            for z in range(2):
                rim = (fl_ref if z == 0 else fh_ref)[o].astype(f32)
                total = int_ref[o, z].astype(f32) + rim + smooth[:, z * SIDE : (z + 1) * SIDE]
                out_ref[o, z] = total.astype(bf16)
        chunk_copy(out_ref, out_hbm, out_sem, k, size).start()
        return carry

    lax.fori_loop(0, CHUNKS, chunk, 0)
    for k in range(CHUNKS):
        chunk_copy(out_ref, out_hbm, out_sem, k, size).wait()


def last(conv_int, from_low, from_high, slab, tables):
    _, _, ext3, eyh, eyl = tables
    return whole(
        last_kernel, ("hbm", "vmem", "vmem", None, None, None, None), ((OWN_FIELD, bf16, "hbm"),),
        [
            pltpu.VMEM(OWN_FIELD, bf16),
            pltpu.VMEM(OWN_FIELD, bf16),
            pltpu.VMEM((OWN * 2 * 16, SIDE), f32),
            pltpu.SemaphoreType.DMA((CHUNKS,)),
            pltpu.SemaphoreType.DMA((CHUNKS,)),
        ],
        conv_int, from_low, from_high, slab, ext3, eyh, eyl,
    )


def ring(axis, step):
    count = lax.axis_size(axis)
    return [(i, (i + step) % count) for i in range(count)]


def swap(value, bits):
    count = lax.axis_size("col")
    return lax.ppermute(value, "col", [(i, i ^ bits) for i in range(count)])


def exchange(value):
    return lax.all_to_all(value, "gz", 0, 0, tiled=True)


def columns_of(mixed, table_z, groups):
    columns = jnp.einsum("jz,cjm->zcm", table_z, mixed, precision=highest)
    return columns.reshape(groups, -1, SIDE)


def step(features, grad_out, conv_weight, spectral_weight):
    plane_count = features.shape[1]
    groups = lax.axis_size("gz")
    table_x = basis(SIDE, 16)
    table_y = basis(SIDE, 16)
    table_z = basis(plane_count * groups, 16)
    exh, exl = host_split(table_x)
    eyh, eyl = host_split(table_y)
    ex2 = np.concatenate([exh, exl], axis=0)
    ey2 = np.concatenate([eyh, eyh], axis=1)
    ext3 = np.concatenate([exh.T, exl.T, exh.T], axis=1)
    eyh, eyl = (np.repeat(t.reshape(2, 1, 8, SIDE), OWN, axis=1).reshape(256, SIDE) for t in (eyh, eyl))
    tables = (ex2, ey2, ext3, eyh, eyl)

    kernel = conv_weight.reshape(OWN, ALL, 3, 3, 3)
    w_forward = jnp.transpose(kernel, (2, 4, 0, 3, 1)).reshape(9 * OWN, 3 * ALL)
    pieces = jnp.stack([conv_weight] + [swap(conv_weight, bits) for bits in range(1, 4)])
    back = lax.dynamic_slice_in_dim(pieces, lax.axis_index("col") * OWN, OWN, 2)
    back = back.reshape(4, OWN, OWN, 3, 3, 3)
    w_back = jnp.transpose(back, (3, 5, 2, 4, 0, 1)).reshape(9 * OWN, 3 * ALL)

    planes = analyse(features, ex2, ey2)
    planes = exchange(planes.reshape(groups, 8, 2 * ALL))
    xt, conv_int, rim_low, rim_high = front(features, w_forward)
    up, down = ring("gz", 1), ring("gz", -1)
    from_low = lax.ppermute(rim_high, "gz", up)
    from_high = lax.ppermute(rim_low, "gz", down)

    table_gz = table_z.reshape(16, groups, plane_count)
    spectrum = jnp.einsum(
        "jgz,gmzc->cjm", table_gz, planes.reshape(groups, 8, plane_count, ALL), precision=highest
    )
    weights32 = spectral_weight.astype(f32)
    mixed = jnp.sum(weights32 * spectrum[:, None], axis=0)
    slab = exchange(columns_of(mixed, table_z, groups)).reshape(2 * groups, SIDE)
    conv_int, w_back = lax.optimization_barrier((conv_int, w_back))
    layer_out, gt, gt_first, gt_last, grad_planes = middle(conv_int, from_low, from_high, slab, grad_out, tables)

    g_low = lax.ppermute(gt_last, "gz", up)
    g_high = lax.ppermute(gt_first, "gz", down)
    g1 = swap(gt, 1)
    g2 = swap(gt, 2)
    local_grad = kernel_grad(xt, gt, g_low, g_high)
    local_grad = local_grad.reshape(groups, -1, SIDE)
    packed = jnp.concatenate([grad_planes.astype(bf16).reshape(groups, 2, SIDE), local_grad], axis=1)
    packed = exchange(packed)
    g2, packed = lax.optimization_barrier((g2, packed))
    scaling = 1.0 / math.sqrt(SIDE * SIDE * plane_count * groups)
    grad_chunk = packed[:, 2:].astype(f32).sum(axis=0) * scaling
    grad_planes = packed[:, :2].astype(f32).reshape(groups, 2, 4, plane_count, OWN)
    g3 = swap(g2, 1)
    grad_modes = jnp.einsum("jgz,grmzc->cjrm", table_gz, grad_planes, precision=highest)
    grad_modes = grad_modes.reshape(OWN, 16, 8)
    back_terms = jnp.sum(weights32 * grad_modes[None], axis=1)
    own = lax.axis_index("col")
    shares = [
        lax.dynamic_slice_in_dim(back_terms, jnp.bitwise_xor(own, bits) * OWN, OWN, 0) for bits in range(4)
    ]
    shares = [swap(share, bits) if bits else share for bits, share in enumerate(shares)]
    back_int, back_low, back_high = back_conv((gt, g1, g2, g3), w_back)
    shares, back_low, back_high = lax.optimization_barrier((shares, back_low, back_high))
    back_modes = sum(shares)
    back_from_low = lax.ppermute(back_high, "gz", up)
    back_from_high = lax.ppermute(back_low, "gz", down)
    grad_spectral = spectrum[:, None] * grad_modes[None]

    columns = columns_of(back_modes, table_z, groups).astype(bf16)
    grad_chunk = jnp.broadcast_to(grad_chunk.astype(bf16), (groups, *grad_chunk.shape))
    packed = exchange(jnp.concatenate([columns, grad_chunk], axis=1))
    slab = packed[:, :2].astype(f32).reshape(2 * groups, SIDE)
    grad_input = last(back_int, back_from_low, back_from_high, slab, tables)

    kernel_sum = packed[:27, 2:].astype(f32).reshape(27, 8, 2, ALL)
    grad_conv = jnp.transpose(kernel_sum, (2, 1, 3, 0)).reshape(OWN, ALL, 27)
    return (layer_out, grad_input, grad_conv, grad_spectral)


def solution(mesh):
    return jax.shard_map(
        step,
        mesh=mesh,
        in_specs=(
            P(None, "gz", None, None),
            P("col", "gz", None, None),
            P("col", None, None),
            P(None, "col", None, "gz"),
        ),
        out_specs=(
            P("col", "gz", None, None),
            P("col", "gz", None, None),
            P("col", None, None),
            P(None, "col", None, "gz"),
        ),
        check_vma=False,
    )
```
